32 devices in a mesh: dp: 4 (over y, core), tensor: 2 (over x), enc: 4 (over z).
Axes of the slice: x: 2, y: 2, z: 4, core: 2. Of those that a mesh axis runs over, the one named last changes fastest.
Arguments:
- span_states: bfloat16 [2048, 8192], P(('dp', 'enc'), 'tensor'), may hold values from -6 to 6
- neighbours: bfloat16 [32, 256, 1024], P(('dp', 'enc'), None, 'tensor'), may hold values from -6 to 6
- lengths: int32 [4], P('dp'), may hold values from 1 to 512, 1024 in all
- wq_enc: bfloat16 [1024, 1024], P('enc', 'tensor')
- wk_enc: bfloat16 [8192, 1024], P('enc', 'tensor'), may hold values from -0.0625 to 0.0625
- wv_enc: bfloat16 [8192, 1024], P('enc', 'tensor'), may hold values from -0.0625 to 0.0625
- wo_enc: bfloat16 [1024, 1024], P('enc', 'tensor'), may hold values from -0.1875 to 0.1875
- wk_dec: bfloat16 [1024, 8192], P(('dp', 'enc'), 'tensor'), may hold values from -0.1875 to 0.1875
- wv_dec: bfloat16 [1024, 8192], P(('dp', 'enc'), 'tensor'), may hold values from -0.1875 to 0.1875
- queries: bfloat16 [2048, 8192], P(('dp', 'enc'), 'tensor'), may hold values from -6 to 6
- grad_out: bfloat16 [2048, 8192], P(('dp', 'enc'), 'tensor'), may hold values from -6 to 6
Outputs:
- attended: bfloat16 [2048, 8192], P(('dp', 'enc'), 'tensor')
- grad_encoded: float32 [32, 256, 1024], P(('dp', 'enc'), None, 'tensor')
The draws below stay inside these ranges and needn't reach their ends.
Inputs may be any that keep to these rules, and one draw needn't show every extreme that they name: `lengths`: some sequence is live over all 512 tokens.
All inputs are finite; a program needn't handle non-finite values. No bound on the sum of `lengths` on one device may be relied on, other than what follows from the above.
Results may differ from the reference program's by a relative error of at most 0.019.
Values may be sent and summed in bfloat16 or wider, within the bound.
No kernel may reach another device: no remote copies, remote signals or barrier semaphores. Data moves between devices by JAX's collectives and lax.ppermute only.
A program may use at most 128 MiB of HBM per device.

```python
import math
import jax
import jax.numpy as jnp
import numpy as np
from jax import lax

D = 8192
HD = 128
DE = 1024
EH = 64
M = 64
NB = 2
R = 128
SEQ_LEN = 512
SEQS = 4
SPANS = 32
TOKENS = 2048


def draw_wq_enc(key, part):
    own_key = jax.random.fold_in(key, 101)
    values = jnp.clip(jax.random.normal(own_key, (DE, DE), jnp.float32), -6.0, 6.0) / math.sqrt(DE)
    return values.astype(jnp.bfloat16)


def draw_queries(key, part):
    own_key = jax.random.fold_in(key, 202)
    values = jnp.clip(jax.random.normal(own_key, (TOKENS, D), jnp.float32), -6.0, 6.0)
    return values.astype(jnp.bfloat16)


def steps_of(stream_key, extent, cuts, least, high):
    loudness = 1.0
    for axis_at, parts in cuts:
        steps = jax.random.uniform(jax.random.fold_in(jax.random.fold_in(stream_key, 6), axis_at), (parts,), jnp.float32, least / len(cuts), high / len(cuts))
        loudness = loudness * jnp.repeat(jnp.exp(steps), extent[axis_at] // parts).reshape((-1,) + (1,) * (len(extent) - 1 - axis_at))
    return loudness


def length_profile(amount, total, bound, lean):
    loads = [(1 << 20) // math.isqrt(standing ** lean) + 1 for standing in range(2, amount + 1)]
    rest, holding = total - bound - (amount - 1), [1] * (amount - 1)
    while rest > 0:
        free = [i for i in range(amount - 1) if holding[i] < bound]
        whole, budget = sum([loads[i] for i in free]), rest
        for i in free:
            more = min(bound - holding[i], max(1, budget * loads[i] // whole), rest)
            holding[i] = holding[i] + more
            rest = rest - more
    return np.array([bound] + holding)


def uneven_parts(stream_key, number_of, total, most, slope):
    if number_of == 2:
        one = jax.random.randint(stream_key, (), max(1, total - most), min(most, total - 1) + 1)
        return jnp.stack([one, total - one])
    tallies = jnp.asarray(length_profile(number_of, total, most, slope), jnp.int32)
    couples = (number_of - 1) // 2
    source_of, sink = tallies[1:1 + 2 * couples:2], tallies[2:2 + 2 * couples:2]
    room = jnp.minimum(source_of - 1, most - sink)
    shifted = jax.random.randint(jax.random.fold_in(stream_key, 1), (couples,), 0, 1 << 20) % (room + 1)
    tallies = tallies.at[1:1 + 2 * couples:2].set(source_of - shifted).at[2:2 + 2 * couples:2].set(sink + shifted)
    return tallies[jax.random.permutation(jax.random.fold_in(stream_key, 2), number_of)]


def normal_values(stream_key, extent, spread, bound, cuts=(), kind=jnp.bfloat16):
    array = jax.random.normal(stream_key, extent, jnp.float32) * spread
    if len(cuts) > 0:
        array = steps_of(stream_key, extent, cuts, -0.22, 0.18) * array
    return jnp.clip(array, min=-bound, max=bound).astype(kind)


def setup_inputs(seed: int = 0) -> dict:
    splits = jax.random.split(jax.random.key(seed), 12)
    return {
        "span_states": normal_values(splits[0], (TOKENS, D), 1.0, 6.0, ((0, 16), (1, 2))),
        "neighbours": normal_values(splits[1], (SPANS, NB * R, DE), 1.0, 6.0, ((0, 16), (2, 2))),
        "lengths": uneven_parts(splits[2], SEQS, SEQS * SEQ_LEN // 2, SEQ_LEN, 2).astype(jnp.int32),
        "wq_enc": draw_wq_enc(jax.random.fold_in(splits[11], 71), 0),
        "wk_enc": normal_values(splits[4], (D, DE), D ** -0.5, 0.0625, ((0, 4), (1, 2))),
        "wv_enc": normal_values(splits[5], (D, DE), D ** -0.5, 0.0625, ((0, 4), (1, 2))),
        "wo_enc": normal_values(splits[6], (DE, DE), DE ** -0.5, 0.1875, ((0, 4), (1, 2))),
        "wk_dec": normal_values(splits[7], (DE, D), DE ** -0.5, 0.1875, ((0, 16), (1, 2))),
        "wv_dec": normal_values(splits[8], (DE, D), DE ** -0.5, 0.1875, ((0, 16), (1, 2))),
        "queries": draw_queries(jax.random.fold_in(splits[11], 71), 0),
        "grad_out": normal_values(splits[10], (TOKENS, D), 1.0, 6.0, ((0, 16), (1, 2))),
    }


def one_sequence(states, neighbour, length, queries, grad_out, wq_enc, wk_enc, wv_enc, wo_enc, wk_dec, wv_dec):
    count = SEQ_LEN // M
    keys_each = NB * R
    flat_neighbour = neighbour.reshape(count * keys_each, DE)
    enc_query = jnp.dot(flat_neighbour, wq_enc, preferred_element_type=jnp.float32).astype(jnp.bfloat16)
    enc_key = jnp.dot(states, wk_enc, preferred_element_type=jnp.float32).astype(jnp.bfloat16)
    enc_value = jnp.dot(states, wv_enc, preferred_element_type=jnp.float32).astype(jnp.bfloat16)
    query_heads = enc_query.reshape(count, keys_each, DE // EH, EH).astype(jnp.float32)
    key_heads = enc_key.reshape(count, M, DE // EH, EH).astype(jnp.float32)
    value_heads = enc_value.reshape(count, M, DE // EH, EH).astype(jnp.float32)
    scores = jnp.einsum('cqhe,ckhe->chqk', query_heads, key_heads) / math.sqrt(EH)
    enc_weights = jax.nn.softmax(scores, axis=-1).astype(jnp.bfloat16)
    head_mix = jnp.einsum('chqk,ckhe->cqhe', enc_weights.astype(jnp.float32), value_heads)
    head_mix = head_mix.astype(jnp.bfloat16).reshape(count * keys_each, DE)
    encoded = flat_neighbour.astype(jnp.float32) + jnp.dot(head_mix, wo_enc, preferred_element_type=jnp.float32)
    encoded = encoded.astype(jnp.bfloat16).reshape(count, keys_each, DE)
    previous = jnp.concatenate([jnp.zeros((1, keys_each, DE), jnp.bfloat16), encoded[:-1]], axis=0)
    previous = previous.reshape(count * keys_each, DE)
    dec_key = jnp.dot(previous, wk_dec, preferred_element_type=jnp.float32).astype(jnp.bfloat16)
    dec_value = jnp.dot(previous, wv_dec, preferred_element_type=jnp.float32).astype(jnp.bfloat16)
    heads_dec = D // HD
    query_dec = queries.reshape(count, M, heads_dec, HD).astype(jnp.float32)
    key_dec = dec_key.reshape(count, keys_each, heads_dec, HD).astype(jnp.float32)
    value_dec = dec_value.reshape(count, keys_each, heads_dec, HD).astype(jnp.float32)
    dec_scores = jnp.einsum('cmhd,ckhd->chmk', query_dec, key_dec) / math.sqrt(HD)
    probs = jax.nn.softmax(dec_scores, axis=-1)
    probs_low = probs.astype(jnp.bfloat16)
    position = jnp.arange(SEQ_LEN, dtype=jnp.int32)
    live_mask = jnp.logical_and(position < length, position >= M).reshape(count, M, 1, 1)
    attended = jnp.einsum('chmk,ckhd->cmhd', probs_low.astype(jnp.float32), value_dec)
    attended = jnp.where(live_mask, attended, 0.0).astype(jnp.bfloat16).reshape(SEQ_LEN, D)
    cotangent = jnp.where(live_mask, grad_out.reshape(count, M, heads_dec, HD), jnp.zeros((), jnp.bfloat16))
    cot_float = cotangent.astype(jnp.float32)
    grad_value = jnp.einsum('chmk,cmhd->ckhd', probs_low.astype(jnp.float32), cot_float).astype(jnp.bfloat16)
    grad_probs = jnp.einsum('cmhd,ckhd->chmk', cot_float, value_dec)
    inner = lax.optimization_barrier(jnp.sum(grad_probs * probs, axis=-1, keepdims=True))
    grad_scores = (probs * (grad_probs - inner) / math.sqrt(HD)).astype(jnp.bfloat16)
    grad_key = jnp.einsum('chmk,cmhd->ckhd', grad_scores.astype(jnp.float32), query_dec).astype(jnp.bfloat16)
    grad_previous = jnp.dot(grad_key.reshape(count * keys_each, D), wk_dec.T, preferred_element_type=jnp.float32)
    grad_previous = grad_previous + jnp.dot(grad_value.reshape(count * keys_each, D), wv_dec.T, preferred_element_type=jnp.float32)
    grad_previous = grad_previous.reshape(count, keys_each, DE)
    grad_encoded = jnp.concatenate([grad_previous[1:], jnp.zeros((1, keys_each, DE), jnp.float32)], axis=0)
    return (attended, grad_encoded)

def reference(span_states, neighbours, lengths, wq_enc, wk_enc, wv_enc, wo_enc, wk_dec, wv_dec, queries, grad_out):
    count = SEQ_LEN // M
    seq_states = span_states.reshape(SEQS, SEQ_LEN, D)
    seq_neighbours = neighbours.reshape(SEQS, count, NB * R, DE)
    seq_queries = queries.reshape(SEQS, SEQ_LEN, D)
    seq_grads = grad_out.reshape(SEQS, SEQ_LEN, D)

    def per_sequence(items):
        return one_sequence(items[0], items[1], items[2], items[3], items[4], wq_enc, wk_enc, wv_enc, wo_enc, wk_dec, wv_dec)
    attended, grad_encoded = lax.map(per_sequence, (seq_states, seq_neighbours, lengths, seq_queries, seq_grads))
    return (attended.reshape(TOKENS, D), grad_encoded.reshape(SPANS, NB * R, DE))
```

```python
import math

import jax
import jax.numpy as jnp
from jax import lax
from jax.experimental import pallas as pl
from jax.experimental.pallas import tpu as pltpu
from jax.sharding import PartitionSpec as P

HD = 128
EH = 64
F32 = jnp.float32
BF16 = jnp.bfloat16


def dot(a, b):
    return lax.dot_general(a, b, (((1,), (0,)), ((), ())), preferred_element_type=F32)


def dot_nt(a, b):
    return lax.dot_general(a, b, (((1,), (1,)), ((), ())), preferred_element_type=F32)


def dot_tn(a, b):
    return lax.dot_general(a, b, (((0,), (0,)), ((), ())), preferred_element_type=F32)


def from_behind(value, axis, steps):
    count = lax.axis_size(axis)
    first, last = (max(0, -steps), min(count, count - steps))
    return lax.ppermute(value, axis, [(source, source + steps) for source in range(first, last)])


def swap(value, axis, mask):
    count = lax.axis_size(axis)
    return lax.ppermute(value, axis, [(i, i ^ mask) for i in range(count)])


def gather_columns(value, axis):
    if lax.axis_size(axis) != 2:
        return lax.all_gather(value, axis, axis=1, tiled=True)
    other = swap(value, axis, 1)
    first = lax.axis_index(axis) == 0
    return jnp.concatenate(
        [jnp.where(first, value, other), jnp.where(first, other, value)], axis=1
    )


def encoder_kernel(q_ref, k_ref, v_ref, n_ref, wo_ref, out_ref, mix_ref, *, spans, keys, span_len):
    pair = 128
    lane = lax.broadcasted_iota(jnp.int32, (span_len, pair), 1)
    low_rows = lane < EH
    low = lax.broadcasted_iota(jnp.int32, (keys, pair), 1) < span_len
    zero = jnp.zeros((), F32)

    def split(x):
        wide = x.astype(F32)
        both = [jnp.where(low_rows, wide, zero), jnp.where(low_rows, zero, wide)]
        return jnp.concatenate(both, axis=0).astype(BF16)

    for c in range(spans):
        for h in range(q_ref.shape[1] // pair):
            cols = pl.ds(h * pair, pair)
            q = q_ref[pl.ds(c * keys, keys), cols]
            k = split(k_ref[pl.ds(c * span_len, span_len), cols])
            v = split(v_ref[pl.ds(c * span_len, span_len), cols])
            s = dot_nt(q, k) * (1.0 / math.sqrt(EH))
            top_low = jnp.max(jnp.where(low, s, -jnp.inf), axis=1, keepdims=True)
            top_high = jnp.max(jnp.where(low, -jnp.inf, s), axis=1, keepdims=True)
            e = jnp.exp(s - jnp.where(low, top_low, top_high))
            sum_low = jnp.sum(jnp.where(low, e, zero), axis=1, keepdims=True)
            sum_high = jnp.sum(jnp.where(low, zero, e), axis=1, keepdims=True)
            w = (e * jnp.where(low, 1.0 / sum_low, 1.0 / sum_high)).astype(BF16)
            mix_ref[pl.ds(c * keys, keys), cols] = dot(w, v).astype(BF16)
    out_ref[...] = (n_ref[...].astype(F32) + dot(mix_ref[...], wo_ref[...])).astype(BF16)


def decoder_kernel(
    meta_ref, prev_ref, wk_ref, wv_ref, q_ref, go_ref, att_ref, gp_ref, dk_ref, dv_ref,
    *, spans, keys, span_len,
):
    scale = 1.0 / math.sqrt(HD)
    prev = prev_ref[...]
    k_all = dot(prev, wk_ref[...]).astype(BF16)
    v_all = dot(prev, wv_ref[...]).astype(BF16)
    for c in range(spans):
        position = (
            meta_ref[0] + c * span_len + lax.broadcasted_iota(jnp.int32, (span_len, HD), 0)
        )
        live = jnp.logical_and(position < meta_ref[1], position >= span_len)
        rows = pl.ds(c * span_len, span_len)
        key_rows = pl.ds(c * keys, keys)
        for h in range(q_ref.shape[1] // HD):
            cols = pl.ds(h * HD, HD)
            q = q_ref[rows, cols]
            k = k_all[c * keys:(c + 1) * keys, h * HD:(h + 1) * HD]
            v = v_all[c * keys:(c + 1) * keys, h * HD:(h + 1) * HD]
            s = dot_nt(q, k) * scale
            e = jnp.exp(s - jnp.max(s, axis=1, keepdims=True))
            p = e * (1.0 / jnp.sum(e, axis=1, keepdims=True))
            low = p.astype(BF16)
            att_ref[rows, cols] = jnp.where(live, dot(low, v), 0.0).astype(BF16)
            ct = jnp.where(live, go_ref[rows, cols].astype(F32), 0.0).astype(BF16)
            dv_ref[key_rows, cols] = dot_tn(low, ct).astype(BF16)
            gp = dot_nt(ct, v)
            inner = jnp.sum(gp * p, axis=1, keepdims=True)
            gs = (p * (gp - inner) * scale).astype(BF16)
            dk_ref[key_rows, cols] = dot_tn(gs, q).astype(BF16)
    total = dot_nt(dk_ref[...], wk_ref[...]) + dot_nt(dv_ref[...], wv_ref[...])

    @pl.when(pl.program_id(0) == 0)
    def _():
        gp_ref[...] = total

    @pl.when(pl.program_id(0) > 0)
    def _():
        gp_ref[...] += total


def encoder_attention(q, k, v, n, wo, spans):
    key_rows, full = q.shape
    body = lambda *refs: encoder_kernel(
        *refs, spans=spans, keys=key_rows // spans, span_len=k.shape[0] // spans
    )
    return pl.pallas_call(
        body,
        out_shape=jax.ShapeDtypeStruct((key_rows, full), BF16),
        scratch_shapes=[pltpu.VMEM((key_rows, full), BF16)],
        name="encoder_attention",
    )(q, k, v, n, wo)


def decoder(meta, prev, wk, wv, q, go, spans):
    key_rows, full = prev.shape
    row_count, width = q.shape
    block = math.gcd(512, width)
    body = lambda *refs: decoder_kernel(
        *refs, spans=spans, keys=key_rows // spans, span_len=row_count // spans
    )
    return pl.pallas_call(
        body,
        grid_spec=pltpu.PrefetchScalarGridSpec(
            num_scalar_prefetch=1,
            grid=(width // block,),
            in_specs=[
                pl.BlockSpec((key_rows, full), lambda i, m: (0, 0)),
                pl.BlockSpec((full, block), lambda i, m: (0, i)),
                pl.BlockSpec((full, block), lambda i, m: (0, i)),
                pl.BlockSpec((row_count, block), lambda i, m: (0, i)),
                pl.BlockSpec((row_count, block), lambda i, m: (0, i)),
            ],
            out_specs=[
                pl.BlockSpec((row_count, block), lambda i, m: (0, i)),
                pl.BlockSpec((key_rows, full), lambda i, m: (0, 0)),
            ],
            scratch_shapes=[
                pltpu.VMEM((key_rows, block), BF16),
                pltpu.VMEM((key_rows, block), BF16),
            ],
        ),
        out_shape=[
            jax.ShapeDtypeStruct((row_count, width), BF16),
            jax.ShapeDtypeStruct((key_rows, full), F32),
        ],
        name="decoder",
    )(meta, prev, wk, wv, q, go)


def full_square(weights, axes_of):
    dp, tensor, enc = axes_of
    shards = lax.axis_size(dp)
    rows, cols = weights[0].shape
    part = rows // shards
    at = lax.axis_index(dp) * part
    mine = jnp.stack([lax.dynamic_slice_in_dim(w, at, part, 0) for w in weights])
    every = lax.all_gather(mine, (enc, dp, tensor), axis=0, tiled=False)
    every = every.reshape(
        lax.axis_size(enc), shards, lax.axis_size(tensor), len(weights), part, cols
    )
    full = every.transpose(3, 0, 1, 4, 2, 5)
    return full.reshape(len(weights), lax.axis_size(enc) * rows, lax.axis_size(tensor) * cols)


def on_device(
    span_states,
    neighbours,
    lengths,
    wq_enc,
    wk_enc,
    wv_enc,
    wo_enc,
    wk_dec,
    wv_dec,
    queries,
    grad_out,
):
    spans, keys_each, width = neighbours.shape
    row_count = span_states.shape[0]
    span_len = row_count // spans
    key_rows = spans * keys_each
    here = lax.axis_index("enc")
    parts = lax.axis_size("enc")
    halves = lax.axis_size("tensor")

    full_states = gather_columns(span_states, "tensor")
    block = full_states.shape[1] // parts
    full_rows = parts * row_count
    key_weight = lax.all_gather(wk_dec, ("dp", "enc"), axis=0, tiled=True)
    square = full_square([wq_enc, wo_enc], ("dp", "tensor", "enc"))
    value_weight = lax.all_gather(wv_dec, ("dp", "enc"), axis=0, tiled=True)

    carried = from_behind(neighbours[spans - 1], "enc", 1)
    behind = jnp.concatenate([carried[None], neighbours[: spans - 1]], axis=0)
    behind = gather_columns(behind.reshape(key_rows, width), "tensor")

    weight = jnp.concatenate([wk_enc, wv_enc], axis=1)
    gathered = jnp.zeros((full_rows, block), BF16)
    for mask in range(parts):
        sent = lax.dynamic_slice_in_dim(full_states, (here ^ mask) * block, block, 1)
        got = swap(sent, "enc", mask) if mask else sent
        gathered = lax.dynamic_update_slice_in_dim(gathered, got, (here ^ mask) * row_count, 0)
    partial = jnp.concatenate([jnp.zeros((span_len, 2 * width), F32), dot(gathered, weight)])
    total = lax.dynamic_slice_in_dim(partial, here * row_count, row_count, 0)
    for mask in range(1, parts):
        sent = lax.dynamic_slice_in_dim(partial, (here ^ mask) * row_count, row_count, 0)
        total = total + swap(sent.astype(BF16), "enc", mask).astype(F32)
    key_value = total.astype(BF16)
    stacked = jnp.concatenate([key_value[:, :width], key_value[:, width:]], axis=0)
    stacked = gather_columns(stacked, "tensor")
    enc_key, enc_value = stacked[:row_count], stacked[row_count:]

    enc_query = dot(behind, square[0]).astype(BF16)
    previous = encoder_attention(enc_query, enc_key, enc_value, behind, square[1], spans)

    meta = jnp.stack([here * row_count, lengths[0]]).astype(jnp.int32)
    attended, grad = decoder(meta, previous, key_weight, value_weight, queries, grad_out, spans)

    first, rest = grad[:keys_each], grad[keys_each:]
    if halves == 2:
        side = lax.axis_index("tensor")
        own = lambda v: lax.dynamic_slice_in_dim(v, side * width, width, 1)
        other = lambda v: lax.dynamic_slice_in_dim(v, (1 - side) * width, width, 1).astype(BF16)
        back = [(i, i - 1) for i in range(1, parts)]
        cross = [
            (s * parts + i, (1 - s) * parts + i - 1) for s in range(2) for i in range(1, parts)
        ]
        from_other = swap(other(rest), "tensor", 1)
        from_next = lax.ppermute(own(first).astype(BF16), "enc", back)
        from_both = lax.ppermute(other(first), ("tensor", "enc"), cross)
        stay = own(rest) + from_other.astype(F32)
        following = from_next.astype(F32) + from_both.astype(F32)
    else:
        summed = lax.psum_scatter(grad.astype(BF16), "tensor", scatter_dimension=1, tiled=True)
        following = from_behind(summed[:keys_each], "enc", -1).astype(F32)
        stay = summed[keys_each:].astype(F32)
    grad_encoded = jnp.concatenate([stay, following], axis=0).reshape(spans, keys_each, width)
    return (attended, grad_encoded)


def solution(mesh):
    in_specs = (
        P(("dp", "enc"), "tensor"),
        P(("dp", "enc"), None, "tensor"),
        P("dp"),
        P("enc", "tensor"),
        P("enc", "tensor"),
        P("enc", "tensor"),
        P("enc", "tensor"),
        P(("dp", "enc"), "tensor"),
        P(("dp", "enc"), "tensor"),
        P(("dp", "enc"), "tensor"),
        P(("dp", "enc"), "tensor"),
    )
    out_specs = (P(("dp", "enc"), "tensor"), P(("dp", "enc"), None, "tensor"))
    return jax.shard_map(
        on_device, mesh=mesh, in_specs=in_specs, out_specs=out_specs, check_vma=False
    )
```
